32 devices in a mesh: dp: 8 (over z, y), tensor: 4 (over x, core).
Axes of the slice: x: 2, y: 2, z: 4, core: 2. Of those that a mesh axis runs over, the one named last changes fastest.
Arguments:
- grads: bfloat16 [8, 1024, 28672], P('dp', None, 'tensor'), may hold values from -6 to 6
- errors: bfloat16 [8, 1024, 28672], P('dp', None, 'tensor'), may hold values from -4 to 4
- basis: float32 [28672, 32], P('tensor'), may hold values from -6 to 6
Outputs:
- new_errors: bfloat16 [8, 1024, 28672], P('dp', None, 'tensor')
- p_basis: float32 [1024, 32], P('tensor')
- q_basis: float32 [28672, 32], P('tensor')
The draws below stay inside these ranges and needn't reach their ends.
All inputs are finite; a program needn't handle non-finite values.
Results may differ from the reference program's by a relative error of at most 0.014.
Values may be sent and summed in bfloat16 or wider, within the bound.
A program may use at most 128 MiB of HBM per device.

```python
import jax
import jax.numpy as jnp
from jax import lax

ROWS = 1024
FF = 28672
RANK = 32
N_DP = 8


def steps_of(key, dims, cuts, least, high):
    gain = 1.0
    for axis_at, shards_of in cuts:
        draws = jax.random.uniform(jax.random.fold_in(jax.random.fold_in(key, 6), axis_at), (shards_of,), jnp.float32, least / len(cuts), high / len(cuts))
        gain = gain * jnp.repeat(jnp.exp(draws), dims[axis_at] // shards_of).reshape((-1,) + (1,) * (len(dims) - 1 - axis_at))
    return gain


def bell_draw(stream_key, extent, spread, reach, split=(), kind=jnp.bfloat16):
    drawn = jax.random.normal(stream_key, extent, jnp.float32) * spread
    if len(split) > 0:
        drawn = steps_of(stream_key, extent, split, -0.22, 0.18) * drawn
    return jnp.clip(drawn, min=-reach, max=reach).astype(kind)


def setup_inputs(seed: int = 0) -> dict:
    streams_of = jax.random.split(jax.random.key(seed), 4)
    grads = bell_draw(streams_of[0], (N_DP, ROWS, FF), 1.0, 6.0, ((0, 8), (2, 4)))
    errors = bell_draw(streams_of[1], (N_DP, ROWS, FF), 0.5, 4.0, ((0, 8), (2, 4)))
    basis = bell_draw(streams_of[2], (FF, RANK), 1.0, 6.0, ((0, 4),), jnp.float32)
    return dict(grads=grads, errors=errors, basis=basis)


def combined(grads, errors, index):
    return (grads[index].astype(jnp.float32) + errors[index].astype(jnp.float32)).astype(jnp.bfloat16)

def reference(grads, errors, basis):
    basis_b = basis.astype(jnp.bfloat16)
    replicas = jnp.arange(N_DP)

    def forward(index):
        return jnp.dot(combined(grads, errors, index).astype(jnp.float32), basis_b.astype(jnp.float32), preferred_element_type=jnp.float32)
    p_sum = jnp.sum(lax.map(forward, replicas), axis=0)
    gram = jnp.dot(p_sum.T, p_sum, precision=lax.Precision.HIGHEST)
    lower = jnp.linalg.cholesky(gram)
    p_basis = jax.scipy.linalg.solve_triangular(lower, p_sum.T, lower=True).T
    p_b = p_basis.astype(jnp.bfloat16)

    def backward(index):
        return jnp.dot(combined(grads, errors, index).T.astype(jnp.float32), p_b.astype(jnp.float32), preferred_element_type=jnp.float32)
    q_basis = jnp.sum(lax.map(backward, replicas), axis=0) / N_DP
    approx = jnp.dot(p_b.astype(jnp.float32), q_basis.astype(jnp.bfloat16).T.astype(jnp.float32), preferred_element_type=jnp.float32)

    def leftover(index):
        return (combined(grads, errors, index).astype(jnp.float32) - approx).astype(jnp.bfloat16)
    new_errors = lax.map(leftover, replicas)
    return (new_errors, p_basis, q_basis)
```

```python
import functools

import jax
import jax.numpy as jnp
from jax import lax
from jax.experimental import pallas as pl
from jax.experimental.pallas import tpu as pltpu
from jax.sharding import PartitionSpec as P

F32, BF16 = jnp.float32, jnp.bfloat16
MESH = pl.DeviceIdType.MESH
HIGHEST = lax.Precision.HIGHEST
LANES = 128


def orthonormal(p_rows, gram):
    lower = jnp.linalg.cholesky(gram)
    return jax.scipy.linalg.solve_triangular(lower, p_rows.T, lower=True).T


def plain_on_device(grads, errors, basis):
    matrix = (grads[0].astype(jnp.float32) + errors[0].astype(jnp.float32)).astype(jnp.bfloat16)
    partial_p = jnp.dot(matrix, basis.astype(jnp.bfloat16), preferred_element_type=jnp.float32)
    p_block = lax.psum_scatter(partial_p, "tensor", scatter_dimension=0, tiled=True)
    p_block = lax.psum(p_block, "dp")
    local_gram = jnp.dot(p_block.T, p_block, precision=lax.Precision.HIGHEST)
    gram = lax.psum(local_gram, "tensor")
    p_basis = orthonormal(p_block, gram)
    p_b = lax.all_gather(p_basis.astype(jnp.bfloat16), "tensor", axis=0, tiled=True)
    local_q = lax.dot_general(
        matrix, p_b, (((0,), (0,)), ((), ())), preferred_element_type=jnp.float32
    )
    q_basis = lax.psum(local_q.astype(jnp.bfloat16), "dp").astype(jnp.float32) / lax.axis_size("dp")
    approx = jnp.dot(p_b, q_basis.astype(jnp.bfloat16).T, preferred_element_type=jnp.float32)
    new_errors = (matrix.astype(jnp.float32) - approx).astype(jnp.bfloat16)[None]
    return (new_errors, p_basis, q_basis)


def ds(start, size, align):
    return pl.ds(pl.multiple_of(start, align), size)


def dot(a, b, dims, precision=None):
    return lax.dot_general(a, b, (dims, ((), ())), precision=precision, preferred_element_type=F32)


def inverse_factor(gram):
    n = gram.shape[0]
    rows = lax.broadcasted_iota(jnp.int32, (n, n), 0)
    cols = lax.broadcasted_iota(jnp.int32, (n, n), 1)
    inv = jnp.where(rows == cols, 1.0, 0.0).astype(F32)
    for k in range(n - 1):
        column = jnp.broadcast_to(gram[:, k : k + 1], (n, n))
        factor = jnp.where(rows > k, column / column[k : k + 1, :], 0.0)
        gram = gram - factor * gram[k : k + 1, :]
        inv = inv - factor * inv[k : k + 1, :]
    pivots = jnp.sum(jnp.where(rows == cols, gram, 0.0), axis=1, keepdims=True)
    return inv / jnp.sqrt(pivots)


def exchange_kernel(
    n_dp, n_t,
    grads, errors, basis_t,
    matrix, p_out, q_out,
    err, basis_b, p_send, p_recv, t_buf, g_buf, pb,
    y_send, y_recv, own, z_send, z_recv, q_all,
    g_in, e_in, ps_s, ps_r, t_s, t_r, g_s, g_r, y_s, y_r, z_s, z_r, a_s, a_r, f_s, f_r,
):
    d, t = lax.axis_index("dp"), lax.axis_index("tensor")
    rank, ff = basis_t.shape
    rows = matrix.shape[0]
    block = rows // n_dp
    piece = ff // n_dp
    half = n_dp // 2
    hi, lo = d // 2, lax.rem(d, 2)
    mate = hi * 2 + 1 - lo

    def nth(i, me, n):
        return lax.rem(me + 1 + i, n)

    def load(j):
        at = ds(j * block, block, block)
        return (
            pltpu.make_async_copy(grads.at[at, :], matrix.at[at, :], g_in.at[j]),
            pltpu.make_async_copy(errors.at[at, :], err.at[at, :], e_in.at[j]),
        )

    @pl.loop(0, n_dp)
    def _(i):
        for copy in load(nth(i, d, n_dp)):
            copy.start()

    barrier = pltpu.get_barrier_semaphore()

    @pl.loop(0, n_dp - 1)
    def _(i):
        pl.semaphore_signal(barrier, inc=1, device_id=(nth(i, d, n_dp), t), device_id_type=MESH)

    @pl.loop(0, n_t - 1)
    def _(i):
        pl.semaphore_signal(barrier, inc=1, device_id=(d, nth(i, t, n_t)), device_id_type=MESH)

    basis_b[...] = basis_t[...].astype(BF16)
    pl.semaphore_wait(barrier, n_dp + n_t - 2)

    def remote(src, dst, send, recv, dp, tensor):
        return pltpu.make_async_remote_copy(
            src_ref=src, dst_ref=dst, send_sem=send, recv_sem=recv,
            device_id=(dp, tensor), device_id_type=MESH,
        )

    def partial(j):
        for copy in load(j):
            copy.wait()
        at = ds(j * block, block, block)
        matrix[at, :] = matrix[at, :] + err[at, :]
        return dot(basis_b[...], matrix[at, :], ((1,), (1,)))

    def p_copy(j, slot):
        return remote(p_send.at[j], p_recv.at[slot], ps_s.at[j], ps_r.at[slot], j, t)

    @pl.loop(0, n_dp - 1)
    def _(i):
        j = nth(i, d, n_dp)
        p_send[j] = partial(j)
        p_copy(j, d).start()

    p_recv[d] = partial(d)

    @pl.loop(0, n_dp - 1)
    def _(i):
        j = nth(i, d, n_dp)
        p_copy(j, j).wait_recv()

    total = p_recv[0]
    for j in range(1, n_dp):
        total = total + p_recv[j]
    t_buf[t] = total

    def t_copy(k, slot):
        return remote(t_buf.at[t], t_buf.at[slot], t_s.at[k], t_r.at[slot], d, k)

    @pl.loop(0, n_t - 1)
    def _(i):
        t_copy(nth(i, t, n_t), t).start()

    @pl.loop(0, n_t - 1)
    def _(i):
        k = nth(i, t, n_t)
        remote(t_buf.at[k], t_buf.at[k], t_s.at[k], t_r.at[k], d, k).wait_recv()

    total = t_buf[0]
    for k in range(1, n_t):
        total = total + t_buf[k]
    g_buf[d] = total

    def g_copy(j, slot):
        return remote(g_buf.at[slot], g_buf.at[slot], g_s.at[j], g_r.at[slot], j, t)

    @pl.loop(0, n_dp - 1)
    def _(i):
        g_copy(nth(i, d, n_dp), d).start()

    @pl.loop(0, n_dp - 1)
    def _(i):
        j = nth(i, d, n_dp)
        g_copy(j, j).wait_recv()

    gram = dot(g_buf[0], g_buf[0], ((1,), (1,)), HIGHEST)
    for j in range(1, n_dp):
        gram = gram + dot(g_buf[j], g_buf[j], ((1,), (1,)), HIGHEST)
    inv = inverse_factor(gram)
    for j in range(n_dp):
        p_rows = dot(inv, g_buf[j], ((1,), (0,)), HIGHEST)
        p_out[:, j * block : (j + 1) * block] = p_rows
        pb[:, j * block : (j + 1) * block] = p_rows.astype(BF16)

    def q_piece(k):
        return dot(pb[...], matrix[:, ds(k * piece, piece, LANES)], ((1,), (0,)))

    def y_copy(h):
        return remote(y_send.at[h], y_recv.at[h], y_s.at[h], y_r.at[h], mate, t)

    def z_copy(h, slot):
        return remote(z_send.at[h], z_recv.at[slot], z_s.at[h], z_r.at[slot], h * 2 + lo, t)

    def a_copy(h, slot):
        return remote(q_all.at[slot], q_all.at[slot], a_s.at[h], a_r.at[slot // 2], h * 2 + lo, t)

    def f_copy(slot):
        return remote(q_all.at[slot], q_all.at[slot], f_s.at[slot // 2], f_r.at[slot // 2], mate, t)

    @pl.loop(0, half)
    def _(i):
        h = nth(i, hi, half)
        y_send[h] = q_piece(h * 2 + 1 - lo).astype(BF16)
        y_copy(h).start()

    @pl.loop(0, half)
    def _(i):
        h = nth(i, hi, half)
        own[h] = q_piece(h * 2 + lo)

    @pl.loop(0, half - 1)
    def _(i):
        h = nth(i, hi, half)
        y_copy(h).wait_recv()
        z_send[h] = (own[h] + y_recv[h].astype(F32)).astype(BF16)
        z_copy(h, hi).start()

    y_copy(hi).wait_recv()
    own[hi] = own[hi] + y_recv[hi].astype(F32)

    @pl.loop(0, half - 1)
    def _(i):
        h = nth(i, hi, half)
        z_copy(h, h).wait_recv()
        own[hi] = own[hi] + z_recv[h].astype(F32)

    q_all[d] = (own[hi] / n_dp).astype(BF16)

    @pl.loop(0, half - 1)
    def _(i):
        a_copy(nth(i, hi, half), d).start()

    f_copy(d).start()

    @pl.loop(0, half - 1)
    def _(i):
        h = nth(i, hi, half)
        a_copy(h, h * 2 + lo).wait_recv()
        f_copy(h * 2 + lo).start()

    @pl.loop(0, half)
    def _(h):
        f_copy(h * 2 + 1 - lo).wait_recv()

    for j in range(n_dp):
        q_out[:, j * piece : (j + 1) * piece] = q_all[j]

    @pl.loop(0, n_dp - 1)
    def _(i):
        j = nth(i, d, n_dp)
        p_copy(j, d).wait_send()
        g_copy(j, d).wait_send()

    @pl.loop(0, n_t - 1)
    def _(i):
        t_copy(nth(i, t, n_t), t).wait_send()

    @pl.loop(0, half - 1)
    def _(i):
        h = nth(i, hi, half)
        z_copy(h, hi).wait_send()
        a_copy(h, d).wait_send()

    @pl.loop(0, half)
    def _(h):
        y_copy(h).wait_send()
        f_copy(h * 2 + lo).wait_send()


def output_kernel(n_t, matrix, p_t, q_t, new_errors, p_out, q_out, pb, slots, sems):
    t = lax.axis_index("tensor")
    rows, ff = matrix.shape
    n_slots, _, width = slots.shape
    chunks = ff // width
    tile = 128
    pb[...] = p_t[...].T.astype(BF16)

    def out(i):
        slot = lax.rem(i, n_slots)
        return pltpu.make_async_copy(
            slots.at[slot], new_errors.at[:, ds(i * width, width, LANES)], sems.at[slot]
        )

    @pl.loop(0, chunks)
    def _(i):
        @pl.when(i >= n_slots)
        def _():
            out(i - n_slots).wait()

        slot = lax.rem(i, n_slots)
        columns = ds(i * width, width, LANES)

        @pl.loop(0, rows // tile)
        def _(r):
            at = ds(r * tile, tile, tile)
            approx = dot(pb[at, :], q_t[:, columns], ((1,), (0,)))
            slots[slot, at, :] = (matrix[at, columns].astype(F32) - approx).astype(BF16)

        out(i).start()

    q_out[...] = q_t[...].astype(F32)
    mine = rows // n_t
    p_out[...] = p_t[:, ds(t * mine, mine, LANES)]

    @pl.loop(chunks - n_slots, chunks)
    def _(i):
        out(i).wait()


def on_device(n_dp, n_t, grads, errors, basis):
    _, rows, ff = grads.shape
    rank = basis.shape[1]
    block, piece, half = rows // n_dp, ff // n_dp, n_dp // 2
    vmem = pl.BlockSpec(memory_space=pltpu.VMEM)
    hbm = pl.BlockSpec(memory_space=pl.ANY)
    dma = lambda n: pltpu.SemaphoreType.DMA((n,))
    matrix, p_t, q_t = pl.pallas_call(
        functools.partial(exchange_kernel, n_dp, n_t),
        name="exchange",
        out_shape=(
            pltpu.VMEM((rows, ff), BF16),
            pltpu.VMEM((rank, rows), F32),
            pltpu.VMEM((rank, ff), BF16),
        ),
        in_specs=[hbm, hbm, vmem],
        out_specs=(vmem, vmem, vmem),
        scratch_shapes=[
            pltpu.VMEM((rows, ff), BF16),
            pltpu.VMEM((rank, ff), BF16),
            pltpu.VMEM((n_dp, rank, block), F32),
            pltpu.VMEM((n_dp, rank, block), F32),
            pltpu.VMEM((n_t, rank, block), F32),
            pltpu.VMEM((n_dp, rank, block), F32),
            pltpu.VMEM((rank, rows), BF16),
            pltpu.VMEM((half, rank, piece), BF16),
            pltpu.VMEM((half, rank, piece), BF16),
            pltpu.VMEM((half, rank, piece), F32),
            pltpu.VMEM((half, rank, piece), BF16),
            pltpu.VMEM((half, rank, piece), BF16),
            pltpu.VMEM((n_dp, rank, piece), BF16),
            dma(n_dp), dma(n_dp),
            dma(n_dp), dma(n_dp),
            dma(n_t), dma(n_t),
            dma(n_dp), dma(n_dp),
            dma(half), dma(half),
            dma(half), dma(half),
            dma(half), dma(half),
            dma(half), dma(half),
        ],
        compiler_params=pltpu.CompilerParams(
            collective_id=0, has_side_effects=True, vmem_limit_bytes=36 * 2**20
        ),
    )(grads[0], errors[0], basis.T)
    width = piece
    n_slots = min(4, ff // width)
    new_errors, p_mine, q_full = pl.pallas_call(
        functools.partial(output_kernel, n_t),
        name="output",
        out_shape=(
            jax.ShapeDtypeStruct((rows, ff), BF16),
            jax.ShapeDtypeStruct((rank, rows // n_t), F32),
            jax.ShapeDtypeStruct((rank, ff), F32),
        ),
        in_specs=[vmem, vmem, vmem],
        out_specs=(hbm, vmem, vmem),
        scratch_shapes=[
            pltpu.VMEM((rows, rank), BF16),
            pltpu.VMEM((n_slots, rows, width), BF16),
            dma(n_slots),
        ],
        compiler_params=pltpu.CompilerParams(vmem_limit_bytes=16 * 2**20),
    )(matrix, p_t, q_t)
    return new_errors[None], p_mine.T, q_full.T


def body(n_dp, n_t):
    def run(grads, errors, basis):
        _, rows, ff = grads.shape
        fits = n_dp % 2 == 0 and rows % (n_dp * LANES) == 0 and rows % (n_t * LANES) == 0
        if fits and ff % (n_dp * LANES) == 0:
            return on_device(n_dp, n_t, grads, errors, basis)
        return plain_on_device(grads, errors, basis)

    return run


def solution(mesh):
    return jax.shard_map(
        body(mesh.shape["dp"], mesh.shape["tensor"]),
        mesh=mesh,
        in_specs=(P("dp", None, "tensor"), P("dp", None, "tensor"), P("tensor", None)),
        out_specs=(P("dp", None, "tensor"), P("tensor", None), P("tensor", None)),
        check_vma=False,
    )
```
